512 devices in a mesh: slide: 2 (over y), row: 64 (over z, core), col: 4 (over x).
Axes of the slice: x: 4, y: 2, z: 32, core: 2. Of those that a mesh axis runs over, the one named last changes fastest.
The devices are a block of a 4x8x32 slice.
Arguments:
- features: bfloat16 [896, 1792, 96], P(('slide', 'row'), 'col'), parts along dimension 0, may hold values from -6 to 6
- region_ids: int32 [128, 256, 49], P(('slide', 'row'), 'col'), parts along dimension 0, may hold values from 0 to 1073741823, as said below
- qkv_weight: bfloat16 [96, 288], replicated, may hold values from -0.625 to 0.625
- proj_weight: bfloat16 [96, 96], replicated, may hold values from -0.625 to 0.625
- rel_bias: float32 [169, 3], replicated, may hold values from -5 to 280
- fc1_weight: bfloat16 [96, 384], replicated, may hold values from -0.625 to 0.625
- fc2_weight: bfloat16 [384, 96], replicated, may hold values from -0.3125 to 0.3125
Outputs:
- block_out: bfloat16 [896, 1792, 96], P(('slide', 'row'), 'col'), parts along dimension 0
The draws below stay inside these ranges and needn't reach their ends.
There are 2 independent parts, one for each index of `slide`. The reference program is written for one: setup_inputs(seed, part) draws one part's arguments, and reference() takes and returns one part's arrays. A program takes and returns all parts, laid end to end along the dimension named above; an argument that names none is the same for every part. Nothing has to cross between parts.
Inputs may be any that keep to these rules, and one draw needn't show every extreme that they name: `region_ids`: within each window, each token's id marks the region it belongs to; a window holds at most 4 distinct ids.
All inputs are finite; a program needn't handle non-finite values.
Results may differ from the reference program's by a relative error of at most 0.011.
Values may be sent and summed in bfloat16 or wider, within the bound.
No kernel may reach another device: no remote copies, remote signals or barrier semaphores. Data moves between devices by JAX's collectives and lax.ppermute only.
A program may use at most 64 MiB of HBM per device.

```python
import jax
import jax.numpy as jnp
import numpy as np
from jax import lax

C = 96
HEADS = 3
HID = 384
WIN = 7
SHIFT = 3
NH = 448
NW = 1792


def draw_region_ids(key, part):
    code_key, row_key, col_key = jax.random.split(jax.random.fold_in(key, 11), 3)
    grid_shape = (NH // WIN, NW // WIN, 1)
    window_code = jax.random.randint(code_key, grid_shape, 0, 2 ** 28) * 4
    cut_row = jax.random.randint(row_key, grid_shape, 0, WIN + 1)
    cut_col = jax.random.randint(col_key, grid_shape, 0, WIN + 1)
    positions = jnp.arange(WIN * WIN)
    below_cut = (positions // WIN >= cut_row).astype(jnp.int32)
    right_cut = (positions % WIN >= cut_col).astype(jnp.int32)
    return (window_code + 2 * below_cut + right_cut).astype(jnp.int32)


def draw_rel_bias(key, part):
    main_key, peak_key = jax.random.split(jax.random.fold_in(key, 23))
    values = jnp.clip(1.5 * jax.random.normal(main_key, ((2 * WIN - 1) * (2 * WIN - 1), HEADS), jnp.float32), -5.0, 5.0)
    return values


def steps_of(stream_key, shape, cuts, low, top_value):
    def one(position, blocks):
        heights = jax.random.uniform(jax.random.fold_in(jax.random.fold_in(stream_key, 6), position), (blocks,), jnp.float32, low / len(cuts), top_value / len(cuts))
        return jnp.repeat(jnp.exp(heights), shape[position] // blocks).reshape((-1,) + (1,) * (len(shape) - position - 1))

    level = one(*cuts[0])
    for cut in cuts[1:]:
        level = level * one(*cut)
    return level


def bell_draw(own_key, extent, scale, bound, cuts=(), dtype=jnp.bfloat16):
    values = scale * jax.random.normal(own_key, extent, jnp.float32)
    if cuts:
        values = values * steps_of(own_key, extent, cuts, -0.22, 0.18)
    return jnp.clip(values, -bound, bound).astype(dtype)


def setup_inputs(seed: int = 0, part: int = 0) -> dict:
    key_of = jax.random.split(jax.random.key(seed), 8)
    part_keys = jax.random.split(jax.random.fold_in(key_of[7], part), 8)
    return {
        "features": bell_draw(part_keys[0], (NH, NW, C), 1.0, 6.0, ((0, 64), (1, 4))),
        "region_ids": draw_region_ids(jax.random.fold_in(jax.random.fold_in(key_of[7], part), 71), part),
        "qkv_weight": bell_draw(key_of[2], (C, 3 * C), C ** -0.5, 0.625),
        "proj_weight": bell_draw(key_of[3], (C, C), C ** -0.5, 0.625),
        "rel_bias": draw_rel_bias(jax.random.fold_in(key_of[7], 71), part),
        "fc1_weight": bell_draw(key_of[5], (C, HID), C ** -0.5, 0.625),
        "fc2_weight": bell_draw(key_of[6], (HID, C), HID ** -0.5, 0.3125),
    }


epsilon = 1e-05

def layer_norm(values):
    average = lax.optimization_barrier(jnp.mean(values, axis=-1, keepdims=True))
    centred = values - average
    variance = lax.optimization_barrier(jnp.mean(centred * centred, axis=-1, keepdims=True))
    return centred * lax.rsqrt(variance + epsilon)

def relative_onehot():
    positions = np.arange(WIN * WIN)
    row_of = positions // WIN
    col_of = positions % WIN
    index = (row_of[:, None] - row_of[None, :] + WIN - 1) * (2 * WIN - 1) + (col_of[:, None] - col_of[None, :] + WIN - 1)
    table = np.zeros((WIN ** 4, (2 * WIN - 1) ** 2), np.float32)
    table[np.arange(WIN ** 4), index.reshape(-1)] = 1.0
    return table

def window_attention(normed_tile, window_ids, qkv_weight, proj_weight, pos_bias):
    tile_rows, tile_cols, width = normed_tile.shape
    win_rows = tile_rows // WIN
    win_cols = tile_cols // WIN
    window_count = win_rows * win_cols
    head_dim = width // HEADS
    windows = normed_tile.reshape(win_rows, WIN, win_cols, WIN, width).transpose(0, 2, 1, 3, 4).reshape(window_count * WIN * WIN, width)
    projected = jnp.dot(windows, qkv_weight, preferred_element_type=jnp.float32).astype(jnp.bfloat16)
    projected = projected.reshape(window_count, WIN * WIN, 3, HEADS, head_dim)
    queries = projected[:, :, 0].astype(jnp.float32)
    key_rows = projected[:, :, 1].astype(jnp.float32)
    value_rows = projected[:, :, 2].astype(jnp.float32)
    scores = jnp.einsum('wihd,wjhd->whij', queries, key_rows) * head_dim ** (-0.5) + pos_bias[None]
    flat_ids = window_ids.reshape(window_count, WIN * WIN)
    allowed = flat_ids[:, None, :, None] == flat_ids[:, None, None, :]
    scores = jnp.where(allowed, scores, -jnp.inf)
    weights = jax.nn.softmax(scores, axis=-1).astype(jnp.bfloat16)
    context = jnp.einsum('whij,wjhd->wihd', weights.astype(jnp.float32), value_rows).astype(jnp.bfloat16)
    context = context.reshape(window_count * WIN * WIN, width)
    result = jnp.dot(context, proj_weight, preferred_element_type=jnp.float32).astype(jnp.bfloat16)
    return result.reshape(win_rows, win_cols, WIN, WIN, width).transpose(0, 2, 1, 3, 4).reshape(tile_rows, tile_cols, width)

def feed_forward(residual_sum, fc1_weight, fc2_weight):
    normed_two = layer_norm(residual_sum).astype(jnp.bfloat16)
    hidden = jax.nn.gelu(jnp.dot(normed_two, fc1_weight, preferred_element_type=jnp.float32), approximate=False).astype(jnp.bfloat16)
    return (residual_sum + jnp.dot(hidden, fc2_weight, preferred_element_type=jnp.float32)).astype(jnp.bfloat16)

def reference(features, region_ids, qkv_weight, proj_weight, rel_bias, fc1_weight, fc2_weight):
    pos_bias = jnp.dot(jnp.asarray(relative_onehot()), rel_bias, precision=lax.Precision.HIGHEST)
    pos_bias = pos_bias.reshape(WIN * WIN, WIN * WIN, HEADS).transpose(2, 0, 1)
    rolled = jnp.roll(features, (-SHIFT, -SHIFT), (0, 1))
    bands = rolled.reshape(NH // WIN, WIN, NW, C)

    def attend_band(inputs):
        band, band_ids = inputs
        normed = layer_norm(band.astype(jnp.float32)).astype(jnp.bfloat16)
        return window_attention(normed, band_ids[None], qkv_weight, proj_weight, pos_bias)
    attended = lax.map(attend_band, (bands, region_ids)).reshape(NH, NW, C)
    attended = jnp.roll(attended, (SHIFT, SHIFT), (0, 1))

    def mlp_band(inputs):
        band, branch_band = inputs
        residual_sum = band.astype(jnp.float32) + branch_band.astype(jnp.float32)
        return feed_forward(residual_sum, fc1_weight, fc2_weight)
    result = lax.map(mlp_band, (features.reshape(NH // WIN, WIN * NW, C), attended.reshape(NH // WIN, WIN * NW, C)))
    return result.reshape(NH, NW, C)
```

```python
import functools

import jax
import jax.numpy as jnp
import numpy as np
from jax import lax
from jax.experimental import pallas as pl
from jax.experimental.pallas import tpu as pltpu
from jax.sharding import PartitionSpec as P

HEADS = 3
WIN = 7
SHIFT = 3
KEEP = WIN - SHIFT
PAD = 8
KEYS = WIN * PAD
GROUP = 5
LANES = 128
NEG = -1e30
F32 = jnp.float32
BF16 = jnp.bfloat16

epsilon = 1e-05


def moved(value, axis, steps):
    count = lax.axis_size(axis)
    pairs = [(source, (source + steps) % count) for source in range(count)]
    return lax.ppermute(value, axis, pairs)


def layer_norm(values):
    average = jnp.mean(values, axis=-1, keepdims=True)
    centred = values - average
    variance = jnp.mean(centred * centred, axis=-1, keepdims=True)
    return centred * lax.rsqrt(variance + epsilon)


def bias_of(rel_bias, first, rows):
    index = np.full((KEYS, rows * PAD), -1, np.int32)
    for kr in range(WIN):
        for kc in range(WIN):
            for qr in range(rows):
                for qc in range(WIN):
                    index[kr * PAD + kc, qr * PAD + qc] = (qr + first - kr + WIN - 1) * (2 * WIN - 1) + (qc - kc + WIN - 1)
    chosen = jnp.asarray(index)[:, None, :] == jnp.arange(rel_bias.shape[0], dtype=jnp.int32)[None, :, None]
    table = jnp.einsum("kpq,ph->khq", chosen.astype(F32), rel_bias, precision=lax.Precision.HIGHEST)
    return table.reshape(KEYS, HEADS * rows * PAD)


def slots(ids):
    count = ids.shape[0]
    wide = jnp.pad(ids.reshape(count, WIN, WIN), ((0, 0), (0, 0), (0, PAD - WIN)), constant_values=-1)
    return wide.reshape(count, KEYS)


def query_slots(ids, first, rows):
    return jnp.concatenate([ids[:, first * PAD : (first + rows) * PAD]] * HEADS, axis=1)


def attend(tokens, att, att_row, base, first, rows, ids_k, ids_q, wqkv, wproj, bias, groups):
    count = rows * PAD
    width = wproj.shape[0]
    head_dim = width // HEADS
    scale = head_dim ** (-0.5)
    lane = lax.broadcasted_iota(jnp.int32, (count, width), 1) // head_dim
    blank = jnp.zeros((PAD, width), F32)

    def group(g, carry):
        tiles = []
        for w in range(GROUP):
            at = (g * GROUP + w) * WIN + PAD - KEEP
            for r in range(WIN):
                tiles.append(tokens[base + r, pl.ds(at, PAD), :])
            tiles.append(blank)
        windows = jnp.concatenate(tiles, axis=0).astype(BF16)
        qkv = jnp.dot(windows, wqkv[...], preferred_element_type=F32)
        queries = qkv[:, :width]
        keys = qkv[:, LANES : LANES + width].astype(BF16)
        values = qkv[:, 2 * LANES : 2 * LANES + width].astype(BF16)
        key_ids = ids_k[g].T
        query_ids = ids_q[g]
        stride = (WIN + 1) * PAD
        contexts = []
        for w in range(GROUP):
            top = w * stride
            own = queries[top + first * PAD : top + first * PAD + count]
            split = jnp.concatenate([jnp.where(lane == h, own, 0.0) for h in range(HEADS)], axis=0).astype(BF16)
            scores = lax.dot_general(
                keys[top : top + KEYS], split, (((1,), (1,)), ((), ())), preferred_element_type=F32
            )
            scores = scores * scale + bias[...]
            scores = jnp.where(key_ids[:KEYS, w : w + 1] == query_ids[w : w + 1, :], scores, NEG)
            scores = jnp.exp(scores - jnp.max(scores, axis=0, keepdims=True))
            weights = (scores / jnp.sum(scores, axis=0, keepdims=True)).astype(BF16)
            mixed = lax.dot_general(
                weights, values[top : top + KEYS], (((0,), (0,)), ((), ())), preferred_element_type=F32
            )
            context = mixed[:count]
            for h in range(1, HEADS):
                context = jnp.where(lane == h, mixed[h * count : (h + 1) * count], context)
            contexts.append(context)
        context = jnp.concatenate(contexts, axis=0).astype(BF16)
        branch = jnp.dot(context, wproj[...], preferred_element_type=F32).astype(BF16).astype(F32)
        for w in range(GROUP):
            at = (g * GROUP + w) * WIN + PAD - KEEP
            for r in range(rows):
                top = w * count + r * PAD
                att[att_row + r, pl.ds(at, PAD), :] = branch[top : top + PAD]
        return carry

    lax.fori_loop(0, groups, group, 0)


def block_kernel(own, before, after, left, right, idk_a, idq_a, idk_b, idq_b, wqkv, wproj, bias_a, bias_b, fc1, fc2, out, tokens, att):
    tile_rows, tile_cols, width = own.shape
    total = 2 * WIN

    def normed(values):
        return layer_norm(values.astype(F32)).astype(BF16).astype(F32)

    for r in range(total):
        if r < KEEP:
            source = before[r]
        elif r < KEEP + WIN:
            source = own[r - KEEP]
        else:
            source = after[r - KEEP - WIN]
        tokens[r, PAD : PAD + tile_cols, :] = normed(source)
    tokens[:, PAD - KEEP : PAD, :] = normed(left[...])
    tail = jnp.concatenate([normed(right[...]), jnp.zeros((total, PAD - SHIFT, width), F32)], axis=1)
    tokens[:, PAD + tile_cols : 2 * PAD + tile_cols, :] = tail
    groups = idk_a.shape[0]
    attend(tokens, att, 0, 0, KEEP, SHIFT, idk_b, idq_b, wqkv, wproj, bias_b, groups)
    attend(tokens, att, SHIFT, WIN, 0, KEEP, idk_a, idq_a, wqkv, wproj, bias_a, groups)

    def row(r, carry):
        summed = own[r].astype(F32) + att[r, PAD : PAD + tile_cols, :]
        second = layer_norm(summed).astype(BF16)
        hidden = jnp.dot(second, fc1[...], preferred_element_type=F32)
        hidden = (0.5 * hidden * (1.0 + lax.erf(hidden * (0.5**0.5)))).astype(BF16)
        out[r] = (summed + jnp.dot(hidden, fc2[...], preferred_element_type=F32)).astype(BF16)
        return carry

    lax.fori_loop(0, tile_rows, row, 0)


def shards(features, region_ids, qkv_weight, proj_weight, rel_bias, fc1_weight, fc2_weight):
    tile_rows, tile_cols, width = features.shape
    before = moved(features[SHIFT:], "row", 1)
    ids_before = moved(region_ids, "row", 1)
    after = moved(features[:SHIFT], "row", -1)
    tall = jnp.concatenate([before, features, after], axis=0)
    left = moved(tall[:, -KEEP:], "col", 1)
    right = moved(tall[:, :SHIFT], "col", -1)
    ids = jnp.concatenate([ids_before, region_ids], axis=0)
    ids = jnp.concatenate([moved(ids[:, -1:], "col", 1), ids], axis=1)
    windows = ids.shape[1]
    groups = -(-windows // GROUP)
    ids = slots(ids.reshape(2 * windows, -1)).reshape(2, groups, GROUP, KEYS)
    ids = jnp.pad(ids, ((0, 0), (0, 0), (0, PAD - GROUP), (0, 0)))
    idk_b, idk_a = ids[0], ids[1]
    idq_b = query_slots(idk_b.reshape(-1, KEYS), KEEP, SHIFT).reshape(groups, PAD, -1)
    idq_a = query_slots(idk_a.reshape(-1, KEYS), 0, KEEP).reshape(groups, PAD, -1)
    wqkv = jnp.pad(qkv_weight.reshape(width, 3, width), ((0, 0), (0, 0), (0, LANES - width))).reshape(width, 3 * LANES)
    bias_a = bias_of(rel_bias, 0, KEEP)
    bias_b = bias_of(rel_bias, KEEP, SHIFT)
    return pl.pallas_call(
        block_kernel,
        out_shape=jax.ShapeDtypeStruct(features.shape, BF16),
        scratch_shapes=[
            pltpu.VMEM((2 * WIN, tile_cols + 2 * PAD, width), F32),
            pltpu.VMEM((tile_rows, tile_cols + 2 * PAD, width), F32),
        ],
        compiler_params=pltpu.CompilerParams(vmem_limit_bytes=48 * 1024 * 1024),
    )(features, before, after, left, right, idk_a, idq_a, idk_b, idq_b, wqkv, proj_weight, bias_a, bias_b, fc1_weight, fc2_weight)


def solution(mesh):
    spec = P(("slide", "row"), "col", None)
    return jax.shard_map(
        shards,
        mesh=mesh,
        in_specs=(spec, spec, P(), P(), P(), P(), P()),
        out_specs=spec,
        check_vma=False,
    )
```

```python
import jax
import jax.numpy as jnp
import numpy as np
from jax import lax
from jax.experimental import pallas as pl
from jax.experimental.layout import Layout, with_layout_constraint
from jax.experimental.pallas import tpu as pltpu
from jax.sharding import PartitionSpec as P


HEADS = 3
WIN = 7
SHIFT = 3
KEEP = WIN - SHIFT
PAD = 8
KEYS = WIN * PAD
GROUP = 13
LANES = 128
NEG = -1e30
F32 = jnp.float32
BF16 = jnp.bfloat16

epsilon = 1e-05


def moved(value, rows, cols):
    height, width = lax.axis_size("row"), lax.axis_size("col")
    pairs = [
        (r * width + c, (r + rows) % height * width + (c + cols) % width) for r in range(height) for c in range(width)
    ]
    return lax.ppermute(value, ("row", "col"), pairs)


def rowmajor(value):
    return with_layout_constraint(value, Layout(major_to_minor=tuple(range(value.ndim))))


def digits_of(ids):
    rows = jnp.stack([(ids >> (8 * n)) & 255 for n in range(4)])
    return rows.astype(BF16)


def ids_from(digits):
    whole = digits.astype(jnp.int32)
    return sum(whole[n] << (8 * n) for n in range(4))


def strip_with_ids(strip, ids):
    width = strip.shape[-1]
    digits = jnp.pad(digits_of(ids), ((0, 0), (0, width - ids.shape[0])))
    return jnp.concatenate([strip.reshape(-1, width), digits], axis=0)


def layer_norm(values, axis):
    average = jnp.mean(values, axis=axis, keepdims=True)
    centred = values - average
    variance = jnp.mean(centred * centred, axis=axis, keepdims=True)
    return centred * lax.rsqrt(variance + epsilon)


def bias_of(rel_bias, first, rows):
    index = np.full((rows * PAD, KEYS), -1, np.int32)
    for kr in range(WIN):
        for kc in range(WIN):
            for qr in range(rows):
                for qc in range(WIN):
                    index[qr * PAD + qc, kr * PAD + kc] = (qr + first - kr + WIN - 1) * (2 * WIN - 1) + (qc - kc + WIN - 1)
    chosen = jnp.asarray(index)[:, None, :] == jnp.arange(rel_bias.shape[0], dtype=jnp.int32)[None, :, None]
    table = jnp.einsum("qpk,ph->hqk", chosen.astype(F32), rel_bias, precision=lax.Precision.HIGHEST)
    return table.reshape(HEADS * rows * PAD, KEYS)


def slots(ids):
    count = ids.shape[0]
    wide = jnp.pad(ids.reshape(count, WIN, WIN), ((0, 0), (0, 0), (0, PAD - WIN)), constant_values=-1)
    return wide.reshape(count, KEYS)


def attend(tokens, att, att_row, base, first, rows, ids, wqkv, wproj, bias, groups):
    count = rows * PAD
    width = wproj.shape[0]
    head_dim = width // HEADS
    scale = head_dim ** (-0.5)
    lane = lax.broadcasted_iota(jnp.int32, (count, LANES), 1) // head_dim
    blank = jnp.zeros((PAD, width), F32)
    ones = jnp.ones((KEYS, LANES), BF16)

    def by_head(values):
        chosen = values[:count]
        for h in range(1, HEADS):
            chosen = jnp.where(lane == h, values[h * count : (h + 1) * count], chosen)
        return chosen

    def group(g, carry):
        tiles = []
        for w in range(GROUP):
            at = (g * GROUP + w) * WIN + PAD - KEEP
            for r in range(WIN):
                tiles.append(tokens[base + r, pl.ds(at, PAD), :])
            tiles.append(blank)
        windows = jnp.concatenate(tiles, axis=0).astype(BF16)
        qkv = jnp.dot(windows, wqkv[...], preferred_element_type=F32)
        queries = qkv[:, :LANES]
        keys = qkv[:, LANES : 2 * LANES].astype(BF16)
        values = qkv[:, 2 * LANES :].astype(BF16)
        key_ids = ids[g]
        query_ids = key_ids.T[first * PAD : first * PAD + count]
        stride = (WIN + 1) * PAD
        contexts = []
        for w in range(GROUP):
            top = w * stride
            own = queries[top + first * PAD : top + first * PAD + count]
            split = jnp.concatenate([jnp.where(lane == h, own, 0.0) for h in range(HEADS)], axis=0).astype(BF16)
            scores = lax.dot_general(
                split, keys[top : top + KEYS], (((1,), (1,)), ((), ())), preferred_element_type=F32
            )
            scores = scores * scale + bias[...]
            same = query_ids[:, w : w + 1] == key_ids[w : w + 1, :]
            scores = jnp.where(jnp.concatenate([same] * HEADS, axis=0), scores, NEG)
            scores = jnp.exp(scores - jnp.max(scores, axis=1, keepdims=True)).astype(BF16)
            both = jnp.concatenate([values[top : top + KEYS], ones], axis=1)
            mixed = jnp.dot(scores, both, preferred_element_type=F32)
            contexts.append(by_head(mixed[:, :LANES]) / by_head(mixed[:, LANES:]))
        context = jnp.concatenate(contexts, axis=0)[:, :width].astype(BF16)
        branch = jnp.dot(context, wproj[...], preferred_element_type=F32).astype(BF16).astype(F32)
        for w in range(GROUP):
            at = (g * GROUP + w) * WIN + PAD - KEEP
            for r in range(rows):
                top = w * count + r * PAD
                att[att_row + r, pl.ds(at, PAD), :] = branch[top : top + PAD]
        return carry

    lax.fori_loop(0, groups, group, 0, unroll=True)


def block_kernel(own, before, after, left, right, ids_a, ids_b, wqkv, wproj, bias_a, bias_b, fc1, fc2, out, tokens, att):
    tile_rows, width, tile_cols = own.shape
    total = 2 * WIN

    def normed(values, axis):
        return layer_norm(values.astype(F32), axis).astype(BF16).astype(F32)

    for r in range(total):
        if r < KEEP:
            source = before[r]
        elif r < KEEP + WIN:
            source = own[r - KEEP]
        else:
            source = after[r - KEEP - WIN]
        tokens[r, PAD : PAD + tile_cols, :] = normed(source, 0).T
    tokens[:, PAD - KEEP : PAD, :] = normed(left[...], -1)
    tail = jnp.concatenate([normed(right[...], -1), jnp.zeros((total, PAD - SHIFT, width), F32)], axis=1)
    tokens[:, PAD + tile_cols : 2 * PAD + tile_cols, :] = tail
    groups = ids_a.shape[0]
    attend(tokens, att, 0, 0, KEEP, SHIFT, ids_b, wqkv, wproj, bias_b, groups)
    attend(tokens, att, SHIFT, WIN, 0, KEEP, ids_a, wqkv, wproj, bias_a, groups)

    def row(r, carry):
        summed = own[r].astype(F32) + att[r, PAD : PAD + tile_cols, :].T
        second = layer_norm(summed, 0).astype(BF16)
        hidden = jnp.dot(fc1[...], second, preferred_element_type=F32)
        hidden = (hidden * (1.0 + lax.erf(hidden * (0.5**0.5)))).astype(BF16)
        out[r] = (summed + jnp.dot(fc2[...], hidden, preferred_element_type=F32)).astype(BF16)
        return carry

    lax.fori_loop(0, tile_rows, row, 0, unroll=True)


def shards(features, region_ids, qkv_weight, proj_weight, rel_bias, fc1_weight, fc2_weight):
    tile_rows, tile_cols, width = features.shape
    tile = rowmajor(jnp.swapaxes(features, 1, 2))
    count = region_ids.shape[-1]

    def columns(rows, part):
        return jnp.swapaxes(rowmajor(rows[:, :, part]), 1, 2)

    first, last = slice(0, SHIFT), slice(tile_cols - KEEP, tile_cols)
    before = rowmajor(moved(rowmajor(tile[SHIFT:]), 1, 0))
    ids_before = moved(region_ids, 1, 0)
    corner_left = moved(strip_with_ids(columns(tile[SHIFT:], last), region_ids[0, -1]), 1, 1)
    corner_right = moved(columns(tile[SHIFT:], first), 1, -1)
    after = rowmajor(moved(rowmajor(tile[:SHIFT]), -1, 0))
    tall = jnp.concatenate([columns(tile, last), columns(after, last)], axis=0)
    side_left = moved(strip_with_ids(tall, region_ids[0, -1]), 0, 1)
    side_right = moved(jnp.concatenate([columns(tile, first), columns(after, first)], axis=0), 0, -1)

    def split(packed):
        return packed[:-4].reshape(-1, KEEP, width), ids_from(packed[-4:, :count])

    corner_left, ids_corner = split(corner_left)
    side_left, ids_side = split(side_left)
    left = jnp.concatenate([corner_left, side_left], axis=0)
    right = jnp.concatenate([corner_right, side_right], axis=0)
    ids = jnp.concatenate([ids_before, region_ids], axis=0)
    ids = jnp.concatenate([jnp.stack([ids_corner, ids_side])[:, None], ids], axis=1)
    windows = ids.shape[1]
    groups = -(-windows // GROUP)
    ids = slots(ids.reshape(2 * windows, -1)).reshape(2, groups, GROUP, KEYS)
    ids = jnp.pad(ids, ((0, 0), (0, 0), (0, -GROUP % PAD), (0, 0)))
    wqkv = jnp.pad(qkv_weight.reshape(width, 3, width), ((0, 0), (0, 0), (0, LANES - width))).reshape(width, 3 * LANES)
    bias_a = bias_of(rel_bias, 0, KEEP)
    bias_b = bias_of(rel_bias, KEEP, SHIFT)
    result = pl.pallas_call(
        block_kernel,
        out_shape=jax.ShapeDtypeStruct((tile_rows, width, tile_cols), BF16),
        scratch_shapes=[
            pltpu.VMEM((2 * WIN, tile_cols + 2 * PAD, width), F32),
            pltpu.VMEM((tile_rows, tile_cols + 2 * PAD, width), F32),
        ],
        compiler_params=pltpu.CompilerParams(vmem_limit_bytes=48 * 1024 * 1024),
    )(
        tile,
        before,
        after,
        left,
        right,
        ids[1],
        ids[0],
        wqkv,
        proj_weight,
        bias_a,
        bias_b,
        fc1_weight.T,
        (0.5 * fc2_weight).T,
    )
    return jnp.swapaxes(result, 1, 2)


def solution(mesh):
    spec = P(("slide", "row"), "col", None)
    return jax.shard_map(
        shards,
        mesh=mesh,
        in_specs=(spec, spec, P(), P(), P(), P(), P()),
        out_specs=spec,
        check_vma=False,
    )
```

```python
import jax
import jax.numpy as jnp
import numpy as np
from jax import lax
from jax.experimental import pallas as pl
from jax.experimental.layout import Layout, with_layout_constraint
from jax.experimental.pallas import tpu as pltpu
from jax.sharding import PartitionSpec as P


HEADS = 3
WIN = 7
SHIFT = 3
KEEP = WIN - SHIFT
PAD = 8
KEYS = WIN * PAD
GROUP = 13
LANES = 128
NEG = -1e30
F32 = jnp.float32
BF16 = jnp.bfloat16

epsilon = 1e-05


def moved(value, rows, cols, keep=None):
    height, width = lax.axis_size("row"), lax.axis_size("col")
    pairs = [
        (r * width + c, (r + rows) % height * width + (c + cols) % width)
        for r in range(height)
        for c in range(width)
        if keep is None or keep(r, c)
    ]
    return lax.ppermute(value, ("row", "col"), pairs)


def rowmajor(value):
    return with_layout_constraint(value, Layout(major_to_minor=tuple(range(value.ndim))))


def digits_of(ids):
    rows = jnp.stack([(ids >> (8 * n)) & 255 for n in range(4)])
    return rows.astype(BF16)


def ids_from(digits):
    whole = digits.astype(jnp.int32)
    return sum(whole[n] << (8 * n) for n in range(4))


def layer_norm(values, axis):
    average = jnp.mean(values, axis=axis, keepdims=True)
    centred = values - average
    variance = jnp.mean(centred * centred, axis=axis, keepdims=True)
    return centred * lax.rsqrt(variance + epsilon)


def bias_of(rel_bias):
    index = np.full((KEYS, KEYS), -1, np.int32)
    for kr in range(WIN):
        for kc in range(WIN):
            for qr in range(WIN):
                for qc in range(WIN):
                    index[qr * PAD + qc, kr * PAD + kc] = (qr - kr + WIN - 1) * (2 * WIN - 1) + (qc - kc + WIN - 1)
    chosen = jnp.asarray(index)[:, None, :] == jnp.arange(rel_bias.shape[0], dtype=jnp.int32)[None, :, None]
    return jnp.einsum("qpk,ph->hqk", chosen.astype(F32), rel_bias, precision=lax.Precision.HIGHEST)


def slots(ids, total):
    count = ids.shape[0]
    wide = jnp.pad(ids.reshape(count, WIN, WIN), ((0, 0), (0, 0), (0, PAD - WIN)), constant_values=-1)
    return jnp.pad(wide.reshape(count, KEYS), ((0, total - count), (0, 0)))


def normed(values, axis):
    return layer_norm(values.astype(F32), axis).astype(BF16).astype(F32)


def attend(windows, ids, first, rows, wqkv, wproj, bias):
    count = rows * PAD
    width = wproj.shape[0]
    head_dim = width // HEADS
    scale = head_dim ** (-0.5)
    lane = lax.broadcasted_iota(jnp.int32, (count, LANES), 1) // head_dim
    blank = jnp.zeros((PAD, width), F32)
    ones = jnp.ones((KEYS, LANES), BF16)

    def by_head(values):
        chosen = values[:count]
        for h in range(1, HEADS):
            chosen = jnp.where(lane == h, values[h * count : (h + 1) * count], chosen)
        return chosen

    tokens = jnp.concatenate([tile for window in windows for tile in [*window, blank]], axis=0).astype(BF16)
    qkv = jnp.dot(tokens, wqkv[...], preferred_element_type=F32)
    queries = qkv[:, :LANES]
    keys = qkv[:, LANES : 2 * LANES].astype(BF16)
    values = qkv[:, 2 * LANES :].astype(BF16)
    query_ids = ids.T[first * PAD : first * PAD + count]
    stride = (WIN + 1) * PAD
    contexts = []
    for w in range(len(windows)):
        top = w * stride
        own = queries[top + first * PAD : top + first * PAD + count]
        split = jnp.concatenate([jnp.where(lane == h, own, 0.0) for h in range(HEADS)], axis=0).astype(BF16)
        scores = lax.dot_general(split, keys[top : top + KEYS], (((1,), (1,)), ((), ())), preferred_element_type=F32)
        scores = scores * scale + bias[...]
        same = query_ids[:, w : w + 1] == ids[w : w + 1, :]
        scores = jnp.where(jnp.concatenate([same] * HEADS, axis=0), scores, NEG)
        scores = jnp.exp(scores - jnp.max(scores, axis=1, keepdims=True)).astype(BF16)
        both = jnp.concatenate([values[top : top + KEYS], ones], axis=1)
        mixed = jnp.dot(scores, both, preferred_element_type=F32)
        contexts.append(by_head(mixed[:, :LANES]) / by_head(mixed[:, LANES:]))
    context = jnp.concatenate(contexts, axis=0)[:, :width].astype(BF16)
    return jnp.dot(context, wproj[...], preferred_element_type=F32).astype(BF16).astype(F32)


def attend_row(tokens, att, count, ids, first, rows, wqkv, wproj, bias):
    for start in range(0, count, GROUP):
        members = range(start, min(start + GROUP, count))
        places = [(b + 1) * WIN + PAD - KEEP for b in members]
        windows = [[tokens[r, at : at + PAD, :] for r in range(WIN)] for at in places]
        branch = attend(windows, ids[start : start + 2 * PAD, :], first, rows, wqkv, wproj, bias)
        for w, at in enumerate(places):
            for r in range(rows):
                top = (w * rows + r) * PAD
                att[r, at : at + PAD, :] = branch[top : top + PAD]


def lower_windows(own, after, ids, wqkv, wproj, bias, att, tokens):
    _, tile_cols = own.shape[1:]
    for r in range(WIN):
        source = own[SHIFT + r] if r < KEEP else after[r - KEEP]
        tokens[r, PAD : PAD + tile_cols, :] = normed(source, 0).T
    attend_row(tokens, att, tile_cols // WIN - 1, ids, 0, KEEP, wqkv, wproj, bias)


def early_kernel(late, own, after, ids, wqkv, wproj, bias, att, tokens):
    @pl.when(late[0] == 0)
    def _():
        lower_windows(own, after, ids, wqkv, wproj, bias, att, tokens)


def late_kernel(late, own, after, ids, wqkv, wproj, bias, early, att, tokens):
    @pl.when(late[0] == 0)
    def _():
        att[...] = early[...]

    @pl.when(late[0] != 0)
    def _():
        lower_windows(own, after, ids, wqkv, wproj, bias, att, tokens)


def final_kernel(
    own, before, edge_a, left, right, ids, ids_edge, wqkv, wproj, bias_a, bias_b, fc1, fc2, att_a, out, tokens, att_b, side, rim
):
    tile_rows, width, tile_cols = own.shape
    for r in range(WIN):
        source = before[r] if r < KEEP else own[r - KEEP]
        tokens[r, PAD : PAD + tile_cols, :] = normed(source, 0).T
    halo_left = normed(left[...], -1)
    halo_right = jnp.concatenate([normed(right[...], -1), jnp.zeros((2 * WIN, PAD - SHIFT, width), F32)], axis=1)
    tokens[:, PAD - KEEP : PAD, :] = halo_left[:WIN]
    tokens[:, PAD + tile_cols : 2 * PAD + tile_cols, :] = halo_right[:WIN]
    inner = normed(edge_a[...], -1)
    side[0, :, PAD - KEEP : PAD, :] = halo_left[WIN:]
    side[0, :, PAD:, :] = inner[:, :PAD]
    side[1, :, :PAD, :] = inner[:, PAD:]
    side[1, :, PAD:, :] = halo_right[WIN:]

    attend_row(tokens, att_b, tile_cols // WIN, ids, KEEP, SHIFT, wqkv, wproj, bias_b)
    skip = slice(PAD - KEEP, 2 * PAD - KEEP)
    window = [tokens[r, skip, :] for r in range(WIN)]
    branch = attend([window], ids_edge[:PAD, :], KEEP, SHIFT, wqkv, wproj, bias_b)
    for r in range(SHIFT):
        rim[0, r, skip, :] = branch[r * PAD : (r + 1) * PAD]
        rim[0, r, 2 * PAD - KEEP - 1 : 2 * PAD, :] = att_b[r, 2 * PAD - KEEP - 1 : 2 * PAD, :]
    windows = [[side[n, r, skip, :] for r in range(WIN)] for n in range(2)]
    branch = attend(windows, ids_edge[PAD:, :], 0, KEEP, wqkv, wproj, bias_a)
    for r in range(KEEP):
        low, high = r * PAD, (KEEP + r) * PAD
        rim[0, SHIFT + r, skip, :] = branch[low : low + PAD]
        rim[0, SHIFT + r, 2 * PAD - KEEP - 1 : 2 * PAD, :] = att_a[r, 2 * PAD - KEEP - 1 : 2 * PAD, :]
        rim[1, r, :PAD, :] = att_a[r, tile_cols : tile_cols + PAD, :]
        rim[1, r, skip, :] = branch[high : high + PAD]

    for r in range(tile_rows):
        if r < SHIFT:
            pieces = [rim[0, r, PAD:, :], att_b[r, 2 * PAD : PAD + tile_cols, :]]
        else:
            pieces = [rim[0, r, PAD:, :], att_a[r - SHIFT, 2 * PAD : tile_cols, :], rim[1, r - SHIFT, :PAD, :]]
        summed = own[r].astype(F32) + jnp.concatenate(pieces, axis=0).T
        second = layer_norm(summed, 0).astype(BF16)
        hidden = jnp.dot(fc1[...], second, preferred_element_type=F32)
        hidden = (hidden * (1.0 + lax.erf(hidden * (0.5**0.5)))).astype(BF16)
        out[r] = (summed + jnp.dot(fc2[...], hidden, preferred_element_type=F32)).astype(BF16)


def shards(features, region_ids, qkv_weight, proj_weight, rel_bias, fc1_weight, fc2_weight):
    tile_rows, tile_cols, width = features.shape
    tile = rowmajor(jnp.swapaxes(features, 1, 2))
    count = region_ids.shape[-1]
    windows = region_ids.shape[1]
    own_ids = region_ids[0]
    height = lax.axis_size("row")
    row, col = lax.axis_index("row"), lax.axis_index("col")

    def in_wrap(r, c):
        return r == 0 or r == height - 1 or (r == 1 and c == 0)

    late = (row >= height - 2) | ((row == 0) & (col == 0))
    late = late.astype(jnp.int32).reshape(1)

    def columns(rows, part):
        return jnp.swapaxes(rowmajor(rows[:, :, part]), 1, 2)

    first, last = slice(0, SHIFT), slice(tile_cols - KEEP, tile_cols)
    room = windows + 2 * PAD
    wqkv = jnp.pad(qkv_weight.reshape(width, 3, width), ((0, 0), (0, 0), (0, LANES - width))).reshape(width, 3 * LANES)
    bias = bias_of(rel_bias)
    bias_a = bias[:, : KEEP * PAD].reshape(HEADS * KEEP * PAD, KEYS)
    bias_b = bias[:, KEEP * PAD :].reshape(HEADS * SHIFT * PAD, KEYS)
    ids_a = slots(own_ids, room)
    smem = pl.BlockSpec(memory_space=pltpu.SMEM)
    vmem = pl.BlockSpec(memory_space=pltpu.VMEM)
    att_shape = jax.ShapeDtypeStruct((KEEP, tile_cols + 2 * PAD, width), F32)
    token_scratch = pltpu.VMEM((WIN, tile_cols + 2 * PAD, width), F32)
    params = pltpu.CompilerParams(vmem_limit_bytes=40 * 1024 * 1024)

    def call(kernel, operands):
        return pl.pallas_call(
            kernel,
            out_shape=att_shape,
            in_specs=[smem] + [vmem] * (len(operands) - 1),
            out_specs=vmem,
            scratch_shapes=[token_scratch],
            compiler_params=params,
        )(*operands)

    before = rowmajor(moved(rowmajor(tile[SHIFT:]), 1, 0))
    ids_before = moved(region_ids, 1, 0)
    after_main = rowmajor(moved(rowmajor(tile[:SHIFT]), -1, 0, lambda r, c: not in_wrap(r, c)))
    att = call(early_kernel, [late, tile, after_main, ids_a, wqkv, proj_weight, bias_a])
    after_wrap = rowmajor(moved(rowmajor(tile[:SHIFT]), -1, 0, in_wrap))

    def sides(part):
        after = jnp.where(late[0] != 0, columns(after_wrap, part), columns(after_main, part))
        return jnp.concatenate([columns(before, part), columns(tile, part), after], axis=0)

    digits = jnp.concatenate([digits_of(ids_before[0, -1]), digits_of(own_ids[-1])], axis=0)
    digits = jnp.pad(digits, ((0, 0), (0, width - count)))
    left = moved(jnp.concatenate([sides(last).reshape(-1, width), digits], axis=0), 0, 1)
    right = moved(sides(first), 0, -1)
    att = call(late_kernel, [late, tile, after_wrap, ids_a, wqkv, proj_weight, bias_a, att])

    ids_b = slots(ids_before[0], room)
    digits = left[-8:, :count]
    ids_edge = slots(jnp.stack([ids_from(digits[:4]), ids_from(digits[4:]), own_ids[-1]]), 3)
    ids_edge = jnp.concatenate([jnp.pad(ids_edge[:1], ((0, PAD - 1), (0, 0))), jnp.pad(ids_edge[1:], ((0, PAD - 2), (0, 0)))])
    left = left[:-8].reshape(2 * WIN, KEEP, width)

    def inner(rows):
        return jnp.concatenate([columns(rows, slice(0, PAD)), columns(rows, slice(tile_cols - PAD, tile_cols))], axis=1)

    edge_a = jnp.concatenate([inner(tile[SHIFT:]), jnp.where(late[0] != 0, inner(after_wrap), inner(after_main))], axis=0)
    result = pl.pallas_call(
        final_kernel,
        out_shape=jax.ShapeDtypeStruct((tile_rows, width, tile_cols), BF16),
        scratch_shapes=[
            token_scratch,
            pltpu.VMEM((SHIFT, tile_cols + 2 * PAD, width), F32),
            pltpu.VMEM((2, WIN, 2 * PAD, width), F32),
            pltpu.VMEM((2, WIN, 2 * PAD, width), F32),
        ],
        compiler_params=params,
    )(
        tile,
        before,
        edge_a,
        left,
        right,
        ids_b,
        ids_edge,
        wqkv,
        proj_weight,
        bias_a,
        bias_b,
        fc1_weight.T,
        (0.5 * fc2_weight).T,
        att,
    )
    return jnp.swapaxes(result, 1, 2)


def solution(mesh):
    spec = P(("slide", "row"), "col", None)
    return jax.shard_map(
        shards,
        mesh=mesh,
        in_specs=(spec, spec, P(), P(), P(), P(), P()),
        out_specs=spec,
        check_vma=False,
    )
```

```python
import functools

import jax
import jax.numpy as jnp
import numpy as np
from jax import lax
from jax.experimental import pallas as pl
from jax.experimental.layout import Layout, with_layout_constraint
from jax.experimental.pallas import tpu as pltpu
from jax.sharding import PartitionSpec as P


HEADS = 3
WIN = 7
SHIFT = 3
KEEP = WIN - SHIFT
PAD = 8
KEYS = WIN * PAD
GROUP = 13
LANES = 128
NEG = -1e30
F32 = jnp.float32
BF16 = jnp.bfloat16

epsilon = 1e-05


def moved(value, rows, cols, keep=None):
    slides, height, width = lax.axis_size("slide"), lax.axis_size("row"), lax.axis_size("col")
    pairs = [
        ((s * height + r) * width + c, (s * height + (r + rows) % height) * width + (c + cols) % width)
        for s in range(slides)
        for r in range(height)
        for c in range(width)
        if keep is None or keep(s, r, c)
    ]
    return lax.ppermute(value, ("slide", "row", "col"), pairs)


def rowmajor(value):
    return with_layout_constraint(value, Layout(major_to_minor=tuple(range(value.ndim))))


def layer_norm(values, axis):
    average = jnp.mean(values, axis=axis, keepdims=True)
    centred = values - average
    variance = jnp.mean(centred * centred, axis=axis, keepdims=True)
    return centred * lax.rsqrt(variance + epsilon)


def bias_onehot():
    span = 2 * WIN - 1
    table = np.zeros((span * span, PAD, LANES), np.float32)
    for cq in range(WIN):
        for j in range(span):
            for ck in range(WIN):
                table[(span - 1 - j) * span + cq - ck + WIN - 1, cq, j * PAD + ck] = 1.0
    return table.reshape(span * span, PAD * LANES)


def fill_strip(rel_bias, onehot, strip):
    rest = rel_bias[...]
    picked = 0.0
    for _ in range(3):
        part = lax.reduce_precision(rest, exponent_bits=8, mantissa_bits=7)
        rest = rest - part
        picked = picked + jnp.dot(part.astype(BF16), onehot[...], preferred_element_type=F32)
    for cq in range(PAD):
        strip[:, cq, :] = picked[:, cq * LANES : (cq + 1) * LANES]


def bias_tiles(strip, first, rows):
    tiles = []
    for h in range(HEADS):
        for r in range(first, first + rows):
            tiles.append(strip[h, :, (WIN - 1 - r) * PAD : (WIN - 1 - r) * PAD + KEYS])
    return jnp.concatenate(tiles, axis=0)


def spread_ids(ids, spread):
    spread[...] = jnp.full(spread.shape, -1, jnp.int32)
    for r in range(WIN):
        spread[r * PAD : r * PAD + WIN, : ids.shape[2]] = ids[r * WIN : (r + 1) * WIN, 0, :]
    return spread[...]


def widen(weight, wide):
    width = weight.shape[0]
    wide[...] = jnp.zeros(wide.shape, BF16)
    for n in range(3):
        wide[:, n * LANES : n * LANES + width] = weight[:, n * width : (n + 1) * width]


def normed(values, axis):
    return layer_norm(values.astype(F32), axis).astype(BF16).astype(F32)


def attend(windows, ids_t, first, rows, wqkv, wproj, bias):
    count = rows * PAD
    width = wproj.shape[0]
    head_dim = width // HEADS
    scale = head_dim ** (-0.5)
    lane = lax.broadcasted_iota(jnp.int32, (count, LANES), 1) // head_dim
    blank = jnp.zeros((PAD, width), F32)
    ones = jnp.ones((KEYS, LANES), BF16)

    def by_head(values):
        chosen = values[:count]
        for h in range(1, HEADS):
            chosen = jnp.where(lane == h, values[h * count : (h + 1) * count], chosen)
        return chosen

    tokens = jnp.concatenate([tile for window in windows for tile in [*window, blank]], axis=0).astype(BF16)
    qkv = jnp.dot(tokens, wqkv[...], preferred_element_type=F32)
    queries = qkv[:, :LANES]
    keys = qkv[:, LANES : 2 * LANES].astype(BF16)
    values = qkv[:, 2 * LANES :].astype(BF16)
    ids = ids_t.T
    query_ids = ids_t[first * PAD : first * PAD + count]
    stride = (WIN + 1) * PAD
    contexts = []
    for w in range(len(windows)):
        top = w * stride
        own = queries[top + first * PAD : top + first * PAD + count]
        split = jnp.concatenate([jnp.where(lane == h, own, 0.0) for h in range(HEADS)], axis=0).astype(BF16)
        scores = lax.dot_general(split, keys[top : top + KEYS], (((1,), (1,)), ((), ())), preferred_element_type=F32)
        scores = scores * scale + bias
        same = query_ids[:, w : w + 1] == ids[w : w + 1, :]
        scores = jnp.where(jnp.concatenate([same] * HEADS, axis=0), scores, NEG)
        scores = jnp.exp(scores - jnp.max(scores, axis=1, keepdims=True)).astype(BF16)
        both = jnp.concatenate([values[top : top + KEYS], ones], axis=1)
        mixed = jnp.dot(scores, both, preferred_element_type=F32)
        contexts.append(by_head(mixed[:, :LANES]) / by_head(mixed[:, LANES:]))
    context = jnp.concatenate(contexts, axis=0)[:, :width].astype(BF16)
    return jnp.dot(context, wproj[...], preferred_element_type=F32).astype(BF16).astype(F32)


def attend_row(tokens, att, count, ids_t, first, rows, wqkv, wproj, bias):
    for start in range(0, count, GROUP):
        members = range(start, min(start + GROUP, count))
        places = [(b + 1) * WIN + PAD - KEEP for b in members]
        windows = [[tokens[r, at : at + PAD, :] for r in range(WIN)] for at in places]
        branch = attend(windows, ids_t[:, start : start + 2 * PAD], first, rows, wqkv, wproj, bias)
        for w, at in enumerate(places):
            for r in range(rows):
                top = (w * rows + r) * PAD
                att[r, at : at + PAD, :] = branch[top : top + PAD]


def lower_windows(own, after, ids, weight, wproj, rel_bias, onehot, att, tokens, wqkv, strip, spread):
    _, tile_cols = own.shape[1:]
    widen(weight, wqkv)
    fill_strip(rel_bias, onehot, strip)
    bias = bias_tiles(strip, 0, KEEP)
    ids_t = spread_ids(ids, spread)
    for r in range(WIN):
        source = own[SHIFT + r] if r < KEEP else after[r - KEEP]
        tokens[r, PAD : PAD + tile_cols, :] = normed(source, 0).T
    attend_row(tokens, att, tile_cols // WIN - 1, ids_t, 0, KEEP, wqkv, wproj, bias)


def early_kernel(late, *refs):
    @pl.when(late[0] == 0)
    def _():
        lower_windows(*refs)


def late_kernel(late, early, *refs):
    @pl.when(late[0] == 0)
    def _():
        refs[7][...] = early[...]

    @pl.when(late[0] != 0)
    def _():
        lower_windows(*refs)


def pack_kernel(late, own, before, after_main, after_wrap, ids, ids_before, left, right, spread):
    tile_cols = own.shape[2]
    for r in range(2 * WIN):
        if r < KEEP:
            source = before[r]
        elif r < KEEP + WIN:
            source = own[r - KEEP]
        else:
            source = jnp.where(late[0] != 0, after_wrap[r - KEEP - WIN], after_main[r - KEEP - WIN])
        source = source.astype(F32)
        right[r] = source[:, :LANES].T[:PAD].astype(BF16)
        tail = tile_cols // LANES * LANES
        left[r] = source[:, tail:].T[tile_cols - tail - PAD :].astype(BF16)
    columns = [spread_ids(each, spread)[:, each.shape[2] - 1 : each.shape[2]] for each in (ids_before, ids)]
    lane = lax.broadcasted_iota(jnp.int32, (KEYS, own.shape[1]), 1)
    chosen = jnp.where(lane < 4, columns[0], columns[1])
    digits = ((chosen >> (8 * (lane & 3))) & 255).astype(F32)
    for r in range(WIN):
        left[2 * WIN + r] = digits[r * PAD : (r + 1) * PAD].astype(BF16)


def final_kernel(
    late,
    own,
    before,
    after_main,
    after_wrap,
    left,
    right,
    ids,
    ids_before,
    weight,
    wproj,
    rel_bias,
    onehot,
    fc1,
    fc2,
    att_a,
    out,
    tokens,
    wqkv,
    strip,
    spread,
    att_b,
    side,
    rim,
):
    tile_rows, _, tile_cols = own.shape
    widen(weight, wqkv)
    fill_strip(rel_bias, onehot, strip)
    bias_a = bias_tiles(strip, 0, KEEP)
    bias_b = bias_tiles(strip, KEEP, SHIFT)
    for r in range(WIN):
        source = before[r] if r < KEEP else own[r - KEEP]
        tokens[r, PAD : PAD + tile_cols, :] = normed(source, 0).T
    halo_left = normed(left[: 2 * WIN], -1)
    halo_right = normed(right[...], -1)
    tokens[:, :PAD, :] = halo_left[:WIN]
    tokens[:, PAD + tile_cols :, :] = halo_right[:WIN]
    side[0, :, :PAD, :] = halo_left[WIN:]
    side[1, :, PAD:, :] = halo_right[WIN:]
    tail = tile_cols // LANES * LANES
    for r in range(WIN):
        if r < KEEP:
            source = own[SHIFT + r]
        else:
            source = jnp.where(late[0] != 0, after_wrap[r - KEEP], after_main[r - KEEP])
        side[0, r, PAD:, :] = normed(source[:, :LANES], 0).T[:PAD]
        side[1, r, :PAD, :] = normed(source[:, tail:], 0).T[tile_cols - tail - PAD :]

    windows = ids.shape[2]
    own_last = spread_ids(ids, spread)[:, windows - 1 : windows]
    lane = lax.broadcasted_iota(jnp.int32, (KEYS, LANES), 1)
    digits = jnp.concatenate([left[2 * WIN + r].astype(F32) for r in range(WIN)], axis=0)
    halves = [digits[:, k : k + 1] + 256.0 * digits[:, k + 1 : k + 2] for k in range(0, 8, 2)]
    halves = [half.astype(jnp.int32) for half in halves]
    whole = [halves[2 * n + 1] * 65536 + halves[2 * n] for n in range(2)]
    spare = lax.broadcasted_iota(jnp.int32, (KEYS, LANES), 0) % PAD == WIN
    edge_b = jnp.where(spare, -1, jnp.broadcast_to(whole[0], (KEYS, LANES)))
    edge_a = jnp.where(spare, -1, jnp.where(lane == 0, whole[1], own_last))

    attend_row(tokens, att_b, windows, spread_ids(ids_before, spread), KEEP, SHIFT, wqkv, wproj, bias_b)
    skip = slice(PAD - KEEP, 2 * PAD - KEEP)
    window = [tokens[r, skip, :] for r in range(WIN)]
    branch = attend([window], edge_b, KEEP, SHIFT, wqkv, wproj, bias_b)
    for r in range(SHIFT):
        rim[0, r, skip, :] = branch[r * PAD : (r + 1) * PAD]
        rim[0, r, 2 * PAD - KEEP - 1 : 2 * PAD, :] = att_b[r, 2 * PAD - KEEP - 1 : 2 * PAD, :]
    pair = [[side[n, r, skip, :] for r in range(WIN)] for n in range(2)]
    branch = attend(pair, edge_a, 0, KEEP, wqkv, wproj, bias_a)
    for r in range(KEEP):
        low, high = r * PAD, (KEEP + r) * PAD
        rim[0, SHIFT + r, skip, :] = branch[low : low + PAD]
        rim[0, SHIFT + r, 2 * PAD - KEEP - 1 : 2 * PAD, :] = att_a[r, 2 * PAD - KEEP - 1 : 2 * PAD, :]
        rim[1, r, :PAD, :] = att_a[r, tile_cols : tile_cols + PAD, :]
        rim[1, r, skip, :] = branch[high : high + PAD]

    narrow = (0.5 * fc2[...].astype(F32)).astype(BF16)
    for r in range(tile_rows):
        if r < SHIFT:
            pieces = [rim[0, r, PAD:, :], att_b[r, 2 * PAD : PAD + tile_cols, :]]
        else:
            pieces = [rim[0, r, PAD:, :], att_a[r - SHIFT, 2 * PAD : tile_cols, :], rim[1, r - SHIFT, :PAD, :]]
        summed = own[r].astype(F32) + jnp.concatenate(pieces, axis=0).T
        second = layer_norm(summed, 0).astype(BF16)
        hidden = jnp.dot(fc1[...], second, preferred_element_type=F32)
        hidden = (hidden * (1.0 + lax.erf(hidden * (0.5**0.5)))).astype(BF16)
        out[r] = (summed + jnp.dot(narrow, hidden, preferred_element_type=F32)).astype(BF16)


def shards(features, region_ids, qkv_weight, proj_weight, rel_bias, fc1_weight, fc2_weight):
    tile_rows, tile_cols, width = features.shape
    tile = rowmajor(jnp.swapaxes(features, 1, 2))
    height = lax.axis_size("row")
    slide, row, col = lax.axis_index("slide"), lax.axis_index("row"), lax.axis_index("col")

    def in_wrap(s, r, c):
        return r == 0 or r == height - 1 or (s == 0 and r == 1 and c == 0)

    late = (row >= height - 2) | ((slide == 0) & (row == 0) & (col == 0))
    late = late.astype(jnp.int32).reshape(1)
    onehot = jnp.asarray(bias_onehot(), BF16)
    table = rel_bias.T
    tokens_first = functools.partial(jnp.transpose, axes=(2, 0, 1))
    ids = tokens_first(region_ids)
    att_shape = jax.ShapeDtypeStruct((KEEP, tile_cols + 2 * PAD, width), F32)
    scratch = [
        pltpu.VMEM((WIN, tile_cols + 2 * PAD, width), F32),
        pltpu.VMEM((width, 3 * LANES), BF16),
        pltpu.VMEM((HEADS, PAD, LANES), F32),
        pltpu.VMEM((KEYS, LANES), jnp.int32),
    ]

    def call(kernel, operands, out_shape, scratch_shapes):
        smem, vmem = pl.BlockSpec(memory_space=pltpu.SMEM), pl.BlockSpec(memory_space=pltpu.VMEM)
        return pl.pallas_call(
            kernel,
            out_shape=out_shape,
            in_specs=[smem] + [vmem] * (len(operands) - 1),
            out_specs=jax.tree.map(lambda _: vmem, out_shape),
            scratch_shapes=scratch_shapes,
            compiler_params=pltpu.CompilerParams(vmem_limit_bytes=20 * 1024 * 1024),
        )(*operands)

    before = rowmajor(moved(rowmajor(tile[SHIFT:]), 1, 0))
    ids_before = tokens_first(moved(region_ids, 1, 0))
    after_main = rowmajor(moved(rowmajor(tile[:SHIFT]), -1, 0, lambda s, r, c: not in_wrap(s, r, c)))
    weights = [qkv_weight, proj_weight, table, onehot]
    att = call(early_kernel, [late, tile, after_main, ids, *weights], att_shape, scratch)
    after_wrap = rowmajor(moved(rowmajor(tile[:SHIFT]), -1, 0, in_wrap))
    left, right = call(
        pack_kernel,
        [late, tile, before, after_main, after_wrap, ids, ids_before],
        (
            jax.ShapeDtypeStruct((3 * WIN, PAD, width), BF16),
            jax.ShapeDtypeStruct((2 * WIN, PAD, width), BF16),
        ),
        scratch[-1:],
    )
    left = moved(left, 0, 1)
    right = moved(right, 0, -1)
    att = call(late_kernel, [late, att, tile, after_wrap, ids, *weights], att_shape, scratch)
    result = call(
        final_kernel,
        [late, tile, before, after_main, after_wrap, left, right, ids, ids_before, *weights]
        + [fc1_weight.T, fc2_weight.T, att],
        jax.ShapeDtypeStruct((tile_rows, width, tile_cols), BF16),
        [
            *scratch,
            pltpu.VMEM((SHIFT, tile_cols + 2 * PAD, width), F32),
            pltpu.VMEM((2, WIN, 2 * PAD, width), F32),
            pltpu.VMEM((2, WIN, 2 * PAD, width), F32),
        ],
    )
    return jnp.swapaxes(result, 1, 2)


def solution(mesh):
    spec = P(("slide", "row"), "col", None)
    return jax.shard_map(
        shards,
        mesh=mesh,
        in_specs=(spec, spec, P(), P(), P(), P(), P()),
        out_specs=spec,
        check_vma=False,
    )
```

```python
import functools

import jax
import jax.numpy as jnp
import numpy as np
from jax import lax
from jax.experimental import pallas as pl
from jax.experimental.layout import Layout, with_layout_constraint
from jax.experimental.pallas import tpu as pltpu
from jax.sharding import PartitionSpec as P


HEADS = 3
WIN = 7
SHIFT = 3
KEEP = WIN - SHIFT
PAD = 8
KEYS = WIN * PAD
GROUP = 13
LANES = 128
NEG = -1e30
F32 = jnp.float32
BF16 = jnp.bfloat16

epsilon = 1e-05


def moved(value, rows, cols, keep=None):
    slides, height, width = lax.axis_size("slide"), lax.axis_size("row"), lax.axis_size("col")
    pairs = [
        ((s * height + r) * width + c, (s * height + (r + rows) % height) * width + (c + cols) % width)
        for s in range(slides)
        for r in range(height)
        for c in range(width)
        if keep is None or keep(s, r, c)
    ]
    return lax.ppermute(value, ("slide", "row", "col"), pairs)


def rowmajor(value):
    return with_layout_constraint(value, Layout(major_to_minor=tuple(range(value.ndim))))


def layer_norm(values, axis):
    average = jnp.mean(values, axis=axis, keepdims=True)
    centred = values - average
    variance = jnp.mean(centred * centred, axis=axis, keepdims=True)
    return centred * lax.rsqrt(variance + epsilon)


def bias_onehot():
    span = 2 * WIN - 1
    table = np.zeros((span * span, PAD, LANES), np.float32)
    for cq in range(WIN):
        for j in range(span):
            for ck in range(WIN):
                table[(span - 1 - j) * span + cq - ck + WIN - 1, cq, j * PAD + ck] = 1.0
    return table.reshape(span * span, PAD * LANES)


def fill_strip(rel_bias, onehot, strip):
    rest = rel_bias[...]
    picked = 0.0
    for _ in range(3):
        part = lax.reduce_precision(rest, exponent_bits=8, mantissa_bits=7)
        rest = rest - part
        picked = picked + jnp.dot(part.astype(BF16), onehot[...], preferred_element_type=F32)
    for cq in range(PAD):
        strip[:, cq, :] = picked[:, cq * LANES : (cq + 1) * LANES]


def bias_tiles(strip, first, rows):
    tiles = []
    for h in range(HEADS):
        for r in range(first, first + rows):
            tiles.append(strip[h, :, (WIN - 1 - r) * PAD : (WIN - 1 - r) * PAD + KEYS])
    return jnp.concatenate(tiles, axis=0)


def spread_ids(ids, spread):
    spread[...] = jnp.full(spread.shape, -1, jnp.int32)
    for r in range(WIN):
        spread[r * PAD : r * PAD + WIN, : ids.shape[2]] = ids[r * WIN : (r + 1) * WIN, 0, :]
    return spread[...]


def widen(weight, wide):
    width = weight.shape[0]
    wide[...] = jnp.zeros(wide.shape, BF16)
    for n in range(3):
        wide[:, n * LANES : n * LANES + width] = weight[:, n * width : (n + 1) * width]


def normed(values, axis):
    return layer_norm(values.astype(F32), axis).astype(BF16).astype(F32)


def attend(windows, ids_t, first, rows, wqkv, wproj, bias):
    count = rows * PAD
    width = wproj.shape[0]
    head_dim = width // HEADS
    scale = head_dim ** (-0.5)
    lane = lax.broadcasted_iota(jnp.int32, (count, LANES), 1) // head_dim
    blank = jnp.zeros((PAD, width), F32)
    ones = jnp.ones((KEYS, LANES), BF16)

    def by_head(values):
        chosen = values[:count]
        for h in range(1, HEADS):
            chosen = jnp.where(lane == h, values[h * count : (h + 1) * count], chosen)
        return chosen

    tokens = jnp.concatenate([tile for window in windows for tile in [*window, blank]], axis=0).astype(BF16)
    qkv = jnp.dot(tokens, wqkv[...], preferred_element_type=F32)
    queries = qkv[:, :LANES]
    keys = qkv[:, LANES : 2 * LANES].astype(BF16)
    values = qkv[:, 2 * LANES :].astype(BF16)
    ids = ids_t.T
    query_ids = ids_t[first * PAD : first * PAD + count]
    stride = (WIN + 1) * PAD
    contexts = []
    for w in range(len(windows)):
        top = w * stride
        own = queries[top + first * PAD : top + first * PAD + count]
        split = jnp.concatenate([jnp.where(lane == h, own, 0.0) for h in range(HEADS)], axis=0).astype(BF16)
        scores = lax.dot_general(split, keys[top : top + KEYS], (((1,), (1,)), ((), ())), preferred_element_type=F32)
        scores = scores * scale + bias
        same = query_ids[:, w : w + 1] == ids[w : w + 1, :]
        scores = jnp.where(jnp.concatenate([same] * HEADS, axis=0), scores, NEG)
        scores = jnp.exp(scores - jnp.max(scores, axis=1, keepdims=True)).astype(BF16)
        both = jnp.concatenate([values[top : top + KEYS], ones], axis=1)
        mixed = jnp.dot(scores, both, preferred_element_type=F32)
        contexts.append(by_head(mixed[:, :LANES]) / by_head(mixed[:, LANES:]))
    context = jnp.concatenate(contexts, axis=0)[:, :width].astype(BF16)
    return jnp.dot(context, wproj[...], preferred_element_type=F32).astype(BF16).astype(F32)


def attend_row(tokens, att, count, ids_t, first, rows, wqkv, wproj, bias):
    for start in range(0, count, GROUP):
        members = range(start, min(start + GROUP, count))
        places = [(b + 1) * WIN + PAD - KEEP for b in members]
        windows = [[tokens[r, at : at + PAD, :] for r in range(WIN)] for at in places]
        branch = attend(windows, ids_t[:, start : start + 2 * PAD], first, rows, wqkv, wproj, bias)
        for w, at in enumerate(places):
            for r in range(rows):
                top = (w * rows + r) * PAD
                att[r, at : at + PAD, :] = branch[top : top + PAD]


def lower_windows(own, after, ids, weight, wproj, rel_bias, onehot, att, tokens, wqkv, strip, spread):
    _, tile_cols = own.shape[1:]
    widen(weight, wqkv)
    fill_strip(rel_bias, onehot, strip)
    bias = bias_tiles(strip, 0, KEEP)
    ids_t = spread_ids(ids, spread)
    for r in range(WIN):
        source = own[SHIFT + r] if r < KEEP else after[r - KEEP]
        tokens[r, PAD : PAD + tile_cols, :] = normed(source, 0).T
    attend_row(tokens, att, tile_cols // WIN - 1, ids_t, 0, KEEP, wqkv, wproj, bias)


def early_kernel(late, *refs):
    @pl.when(late[0] == 0)
    def _():
        lower_windows(*refs)


def late_kernel(late, early, *refs):
    @pl.when(late[0] == 0)
    def _():
        refs[7][...] = early[...]

    @pl.when(late[0] != 0)
    def _():
        lower_windows(*refs)


def pack_kernel(late, own, before, after_main, after_wrap, ids, ids_before, left, right, spread):
    tile_cols = own.shape[2]
    for r in range(2 * WIN):
        if r < KEEP:
            source = before[r]
        elif r < KEEP + WIN:
            source = own[r - KEEP]
        else:
            source = jnp.where(late[0] != 0, after_wrap[r - KEEP - WIN], after_main[r - KEEP - WIN])
        source = source.astype(F32)
        right[r] = source[:, :LANES].T[:PAD].astype(BF16)
        tail = tile_cols // LANES * LANES
        left[r] = source[:, tail:].T[tile_cols - tail - PAD :].astype(BF16)
    columns = [spread_ids(each, spread)[:, each.shape[2] - 1 : each.shape[2]] for each in (ids_before, ids)]
    lane = lax.broadcasted_iota(jnp.int32, (KEYS, own.shape[1]), 1)
    chosen = jnp.where(lane < 4, columns[0], columns[1])
    digits = ((chosen >> (8 * (lane & 3))) & 255).astype(F32)
    for r in range(WIN):
        left[2 * WIN + r] = digits[r * PAD : (r + 1) * PAD].astype(BF16)


def upper_kernel(late, own, before, ids_before, weight, wproj, rel_bias, onehot, att, tokens, wqkv, strip, spread):
    tile_cols = own.shape[2]
    widen(weight, wqkv)
    fill_strip(rel_bias, onehot, strip)
    for r in range(WIN):
        source = before[r] if r < KEEP else own[r - KEEP]
        tokens[r, PAD : PAD + tile_cols, :] = normed(source, 0).T
    bias = bias_tiles(strip, KEEP, SHIFT)
    count = tile_cols // WIN - 1
    attend_row(tokens, att, count, spread_ids(ids_before, spread), KEEP, SHIFT, wqkv, wproj, bias)


def final_kernel(
    late,
    own,
    before,
    after_main,
    after_wrap,
    left,
    right,
    ids,
    ids_before,
    weight,
    wproj,
    rel_bias,
    onehot,
    fc1,
    fc2,
    att_a,
    att_b,
    out,
    wqkv,
    strip,
    spread,
    side,
    rim,
):
    tile_rows, _, tile_cols = own.shape
    widen(weight, wqkv)
    fill_strip(rel_bias, onehot, strip)
    bias_a = bias_tiles(strip, 0, KEEP)
    bias_b = bias_tiles(strip, KEEP, SHIFT)
    halo_left = normed(left[: 2 * WIN], -1)
    halo_right = normed(right[...], -1)
    tail = tile_cols // LANES * LANES
    for r in range(2 * WIN):
        if r < KEEP:
            source = before[r]
        elif r < KEEP + WIN:
            source = own[r - KEEP]
        else:
            source = jnp.where(late[0] != 0, after_wrap[r - KEEP - WIN], after_main[r - KEEP - WIN])
        side[0, r, :PAD, :] = halo_left[r]
        side[0, r, PAD:, :] = normed(source[:, :LANES], 0).T[:PAD]
        side[1, r, :PAD, :] = normed(source[:, tail:], 0).T[tile_cols - tail - PAD :]
        side[1, r, PAD:, :] = halo_right[r]

    windows = ids.shape[2]
    lasts = [spread_ids(each, spread)[:, windows - 1 : windows] for each in (ids_before, ids)]
    lane = lax.broadcasted_iota(jnp.int32, (KEYS, LANES), 1)
    digits = jnp.concatenate([left[2 * WIN + r].astype(F32) for r in range(WIN)], axis=0)
    halves = [digits[:, k : k + 1] + 256.0 * digits[:, k + 1 : k + 2] for k in range(0, 8, 2)]
    halves = [half.astype(jnp.int32) for half in halves]
    whole = [halves[2 * n + 1] * 65536 + halves[2 * n] for n in range(2)]
    spare = lax.broadcasted_iota(jnp.int32, (KEYS, LANES), 0) % PAD == WIN
    edge_ids = [jnp.where(spare, -1, jnp.where(lane == 0, whole[n], lasts[n])) for n in range(2)]

    skip = slice(PAD - KEEP, 2 * PAD - KEEP)
    rest = slice(2 * PAD - KEEP - 1, 2 * PAD)
    for n, (first, rows, bias, att) in enumerate(((KEEP, SHIFT, bias_b, att_b), (0, KEEP, bias_a, att_a))):
        pair = [[side[m, n * WIN + r, skip, :] for r in range(WIN)] for m in range(2)]
        branch = attend(pair, edge_ids[n], first, rows, wqkv, wproj, bias)
        for r in range(rows):
            low, high, place = r * PAD, (rows + r) * PAD, n * SHIFT + r
            rim[0, place, skip, :] = branch[low : low + PAD]
            rim[0, place, rest, :] = att[r, rest, :]
            rim[1, place, :PAD, :] = att[r, tile_cols : tile_cols + PAD, :]
            rim[1, place, skip, :] = branch[high : high + PAD]

    narrow = (0.5 * fc2[...].astype(F32)).astype(BF16)
    for r in range(tile_rows):
        inner = att_b[r, 2 * PAD : tile_cols, :] if r < SHIFT else att_a[r - SHIFT, 2 * PAD : tile_cols, :]
        pieces = [rim[0, r, PAD:, :], inner, rim[1, r, :PAD, :]]
        summed = own[r].astype(F32) + jnp.concatenate(pieces, axis=0).T
        second = layer_norm(summed, 0).astype(BF16)
        hidden = jnp.dot(fc1[...], second, preferred_element_type=F32)
        hidden = (hidden * (1.0 + lax.erf(hidden * (0.5**0.5)))).astype(BF16)
        out[r] = (summed + jnp.dot(narrow, hidden, preferred_element_type=F32)).astype(BF16)


def shards(features, region_ids, qkv_weight, proj_weight, rel_bias, fc1_weight, fc2_weight):
    tile_rows, tile_cols, width = features.shape
    tile = rowmajor(jnp.swapaxes(features, 1, 2))
    height = lax.axis_size("row")
    slide, row, col = lax.axis_index("slide"), lax.axis_index("row"), lax.axis_index("col")

    def in_wrap(s, r, c):
        return r == 0 or r == height - 1 or (s == 0 and r == 1 and c == 0)

    late = (row >= height - 2) | ((slide == 0) & (row == 0) & (col == 0))
    late = late.astype(jnp.int32).reshape(1)
    onehot = jnp.asarray(bias_onehot(), BF16)
    table = rel_bias.T
    tokens_first = functools.partial(jnp.transpose, axes=(2, 0, 1))
    ids = tokens_first(region_ids)
    att_shape = jax.ShapeDtypeStruct((KEEP, tile_cols + 2 * PAD, width), F32)
    scratch = [
        pltpu.VMEM((WIN, tile_cols + 2 * PAD, width), F32),
        pltpu.VMEM((width, 3 * LANES), BF16),
        pltpu.VMEM((HEADS, PAD, LANES), F32),
        pltpu.VMEM((KEYS, LANES), jnp.int32),
    ]

    def call(kernel, operands, out_shape, scratch_shapes):
        smem, vmem = pl.BlockSpec(memory_space=pltpu.SMEM), pl.BlockSpec(memory_space=pltpu.VMEM)
        return pl.pallas_call(
            kernel,
            out_shape=out_shape,
            in_specs=[smem] + [vmem] * (len(operands) - 1),
            out_specs=jax.tree.map(lambda _: vmem, out_shape),
            scratch_shapes=scratch_shapes,
            compiler_params=pltpu.CompilerParams(vmem_limit_bytes=20 * 1024 * 1024),
        )(*operands)

    before = rowmajor(moved(rowmajor(tile[SHIFT:]), 1, 0))
    ids_before = tokens_first(moved(region_ids, 1, 0))
    after_main = rowmajor(moved(rowmajor(tile[:SHIFT]), -1, 0, lambda s, r, c: not in_wrap(s, r, c)))
    weights = [qkv_weight, proj_weight, table, onehot]
    att = call(early_kernel, [late, tile, after_main, ids, *weights], att_shape, scratch)
    after_wrap = rowmajor(moved(rowmajor(tile[:SHIFT]), -1, 0, in_wrap))
    left, right = call(
        pack_kernel,
        [late, tile, before, after_main, after_wrap, ids, ids_before],
        (
            jax.ShapeDtypeStruct((3 * WIN, PAD, width), BF16),
            jax.ShapeDtypeStruct((2 * WIN, PAD, width), BF16),
        ),
        scratch[-1:],
    )
    left = moved(left, 0, 1)
    right = moved(right, 0, -1)
    att = call(late_kernel, [late, att, tile, after_wrap, ids, *weights], att_shape, scratch)
    upper = jax.ShapeDtypeStruct((SHIFT, tile_cols + 2 * PAD, width), F32)
    att_b = call(upper_kernel, [late, tile, before, ids_before, *weights], upper, scratch)
    result = call(
        final_kernel,
        [late, tile, before, after_main, after_wrap, left, right, ids, ids_before, *weights]
        + [fc1_weight.T, fc2_weight.T, att, att_b],
        jax.ShapeDtypeStruct((tile_rows, width, tile_cols), BF16),
        [*scratch[1:], pltpu.VMEM((2, 2 * WIN, 2 * PAD, width), F32), pltpu.VMEM((2, WIN, 2 * PAD, width), F32)],
    )
    return jnp.swapaxes(result, 1, 2)


def solution(mesh):
    spec = P(("slide", "row"), "col", None)
    return jax.shard_map(
        shards,
        mesh=mesh,
        in_specs=(spec, spec, P(), P(), P(), P(), P()),
        out_specs=spec,
        check_vma=False,
    )
```

```python
import functools

import jax
import jax.numpy as jnp
import numpy as np
from jax import lax
from jax.experimental import pallas as pl
from jax.experimental.layout import Layout, with_layout_constraint
from jax.experimental.pallas import tpu as pltpu
from jax.sharding import PartitionSpec as P


HEADS = 3
WIN = 7
SHIFT = 3
KEEP = WIN - SHIFT
PAD = 8
KEYS = WIN * PAD
GROUP = 16
LANES = 128
NEG = -1e30
F32 = jnp.float32
BF16 = jnp.bfloat16

epsilon = 1e-05


def moved(value, rows, cols, keep=None):
    slides, height, width = lax.axis_size("slide"), lax.axis_size("row"), lax.axis_size("col")
    pairs = [
        ((s * height + r) * width + c, (s * height + (r + rows) % height) * width + (c + cols) % width)
        for s in range(slides)
        for r in range(height)
        for c in range(width)
        if keep is None or keep(s, r, c)
    ]
    return lax.ppermute(value, ("slide", "row", "col"), pairs)


def rowmajor(value):
    return with_layout_constraint(value, Layout(major_to_minor=tuple(range(value.ndim))))


def layer_norm(values, axis):
    average = jnp.mean(values, axis=axis, keepdims=True)
    centred = values - average
    variance = jnp.mean(centred * centred, axis=axis, keepdims=True)
    return centred * lax.rsqrt(variance + epsilon)


def bias_onehot():
    span = 2 * WIN - 1
    table = np.zeros((span * span, PAD, LANES), np.float32)
    for cq in range(WIN):
        for j in range(span):
            for ck in range(WIN):
                table[(span - 1 - j) * span + cq - ck + WIN - 1, cq, j * PAD + ck] = 1.0
    return table.reshape(span * span, PAD * LANES)


def fill_strip(rel_bias, onehot, strip):
    rest = rel_bias[...]
    picked = 0.0
    for _ in range(3):
        part = lax.reduce_precision(rest, exponent_bits=8, mantissa_bits=7)
        rest = rest - part
        picked = picked + jnp.dot(part.astype(BF16), onehot[...], preferred_element_type=F32)
    for cq in range(PAD):
        strip[:, cq, :] = picked[:, cq * LANES : (cq + 1) * LANES]


def bias_tiles(strip, first, rows):
    tiles = []
    for h in range(HEADS):
        for r in range(first, first + rows):
            tiles.append(strip[h, :, (WIN - 1 - r) * PAD : (WIN - 1 - r) * PAD + KEYS])
    return jnp.concatenate(tiles, axis=0)


def spread_ids(ids, spread):
    spread[...] = jnp.full(spread.shape, -1, jnp.int32)
    for r in range(WIN):
        spread[r * PAD : r * PAD + WIN, : ids.shape[2]] = ids[r * WIN : (r + 1) * WIN, 0, :]
    return spread[...]


def widen(weight, wide):
    width = weight.shape[0]
    wide[...] = jnp.zeros(wide.shape, BF16)
    for n in range(3):
        wide[:, n * LANES : n * LANES + width] = weight[:, n * width : (n + 1) * width]


def normed(values, axis):
    return layer_norm(values.astype(F32), axis).astype(BF16).astype(F32)


def attend(windows, ids_t, first, rows, wqkv, wproj, bias):
    count = rows * PAD
    width = wproj.shape[0]
    head_dim = width // HEADS
    scale = head_dim ** (-0.5)
    lane = lax.broadcasted_iota(jnp.int32, (count, LANES), 1) // head_dim
    blank = jnp.zeros((PAD, width), F32)
    ones = jnp.ones((KEYS, LANES), BF16)

    def by_head(values):
        chosen = values[:count]
        for h in range(1, HEADS):
            chosen = jnp.where(lane == h, values[h * count : (h + 1) * count], chosen)
        return chosen

    tokens = jnp.concatenate([tile for window in windows for tile in [*window, blank]], axis=0).astype(BF16)
    qkv = jnp.dot(tokens, wqkv[...], preferred_element_type=F32)
    queries = qkv[:, :LANES]
    keys = qkv[:, LANES : 2 * LANES].astype(BF16)
    values = qkv[:, 2 * LANES :].astype(BF16)
    ids = ids_t.T
    query_ids = ids_t[first * PAD : first * PAD + count]
    stride = (WIN + 1) * PAD
    contexts = []
    for w in range(len(windows)):
        top = w * stride
        own = queries[top + first * PAD : top + first * PAD + count]
        split = jnp.concatenate([jnp.where(lane == h, own, 0.0) for h in range(HEADS)], axis=0).astype(BF16)
        scores = lax.dot_general(split, keys[top : top + KEYS], (((1,), (1,)), ((), ())), preferred_element_type=F32)
        scores = scores * scale + bias
        same = query_ids[:, w : w + 1] == ids[w : w + 1, :]
        scores = jnp.where(jnp.concatenate([same] * HEADS, axis=0), scores, NEG)
        scores = jnp.exp(scores - jnp.max(scores, axis=1, keepdims=True)).astype(BF16)
        both = jnp.concatenate([values[top : top + KEYS], ones], axis=1)
        mixed = jnp.dot(scores, both, preferred_element_type=F32)
        contexts.append(by_head(mixed[:, :LANES]) / by_head(mixed[:, LANES:]))
    context = jnp.concatenate(contexts, axis=0)[:, :width].astype(BF16)
    return jnp.dot(context, wproj[...], preferred_element_type=F32).astype(BF16).astype(F32)


def attend_row(tokens, att, count, ids_t, first, rows, wqkv, wproj, bias):
    for start in range(0, count, GROUP):
        members = range(start, min(start + GROUP, count))
        places = [(b + 1) * WIN + PAD - KEEP for b in members]
        windows = [[tokens[r, at : at + PAD, :] for r in range(WIN)] for at in places]
        branch = attend(windows, ids_t[:, start : start + 2 * PAD], first, rows, wqkv, wproj, bias)
        for w, at in enumerate(places):
            for r in range(rows):
                top = (w * rows + r) * PAD
                att[r, at : at + PAD, :] = branch[top : top + PAD]


def lower_windows(own, after, ids, weight, wproj, rel_bias, onehot, att, tokens, wqkv, strip, spread):
    _, tile_cols = own.shape[1:]
    widen(weight, wqkv)
    fill_strip(rel_bias, onehot, strip)
    bias = bias_tiles(strip, 0, KEEP)
    ids_t = spread_ids(ids, spread)
    for r in range(WIN):
        source = own[SHIFT + r] if r < KEEP else after[r - KEEP]
        tokens[r, PAD : PAD + tile_cols, :] = normed(source, 0).T
    attend_row(tokens, att, tile_cols // WIN - 1, ids_t, 0, KEEP, wqkv, wproj, bias)


def early_kernel(late, *refs):
    @pl.when(late[0] == 0)
    def _():
        lower_windows(*refs)


def late_kernel(late, *refs):
    @pl.when(late[0] != 0)
    def _():
        lower_windows(*refs)


def pack_kernel(late, own, before, after_main, after_wrap, ids, ids_before, left, right, spread):
    tile_cols = own.shape[2]
    for r in range(2 * WIN):
        if r < KEEP:
            source = before[r]
        elif r < KEEP + WIN:
            source = own[r - KEEP]
        else:
            source = jnp.where(late[0] != 0, after_wrap[r - KEEP - WIN], after_main[r - KEEP - WIN])
        source = source.astype(F32)
        right[r] = source[:, :LANES].T[:PAD].astype(BF16)
        tail = tile_cols // LANES * LANES
        left[r] = source[:, tail:].T[tile_cols - tail - PAD :].astype(BF16)
    columns = [spread_ids(each, spread)[:, each.shape[2] - 1 : each.shape[2]] for each in (ids_before, ids)]
    lane = lax.broadcasted_iota(jnp.int32, (KEYS, own.shape[1]), 1)
    chosen = jnp.where(lane < 4, columns[0], columns[1])
    digits = ((chosen >> (8 * (lane & 3))) & 255).astype(F32)
    for r in range(WIN):
        left[2 * WIN + r] = digits[r * PAD : (r + 1) * PAD].astype(BF16)


def upper_kernel(late, own, before, ids_before, weight, wproj, rel_bias, onehot, att, tokens, wqkv, strip, spread):
    tile_cols = own.shape[2]
    widen(weight, wqkv)
    fill_strip(rel_bias, onehot, strip)
    for r in range(WIN):
        source = before[r] if r < KEEP else own[r - KEEP]
        tokens[r, PAD : PAD + tile_cols, :] = normed(source, 0).T
    bias = bias_tiles(strip, KEEP, SHIFT)
    count = tile_cols // WIN - 1
    attend_row(tokens, att, count, spread_ids(ids_before, spread), KEEP, SHIFT, wqkv, wproj, bias)


def final_kernel(
    late,
    own,
    before,
    after_main,
    after_wrap,
    left,
    right,
    ids,
    ids_before,
    weight,
    wproj,
    rel_bias,
    onehot,
    fc1,
    fc2,
    att_early,
    att_late,
    att_b,
    out,
    wqkv,
    strip,
    spread,
    side,
    rim,
):
    tile_rows, _, tile_cols = own.shape
    widen(weight, wqkv)
    fill_strip(rel_bias, onehot, strip)
    bias_a = bias_tiles(strip, 0, KEEP)
    bias_b = bias_tiles(strip, KEEP, SHIFT)
    halo_left = normed(left[: 2 * WIN], -1)
    halo_right = normed(right[...], -1)
    tail = tile_cols // LANES * LANES
    for r in range(2 * WIN):
        if r < KEEP:
            source = before[r]
        elif r < KEEP + WIN:
            source = own[r - KEEP]
        else:
            source = jnp.where(late[0] != 0, after_wrap[r - KEEP - WIN], after_main[r - KEEP - WIN])
        side[0, r, :PAD, :] = halo_left[r]
        side[0, r, PAD:, :] = normed(source[:, :LANES], 0).T[:PAD]
        side[1, r, :PAD, :] = normed(source[:, tail:], 0).T[tile_cols - tail - PAD :]
        side[1, r, PAD:, :] = halo_right[r]

    windows = ids.shape[2]
    lasts = [spread_ids(each, spread)[:, windows - 1 : windows] for each in (ids_before, ids)]
    lane = lax.broadcasted_iota(jnp.int32, (KEYS, LANES), 1)
    digits = jnp.concatenate([left[2 * WIN + r].astype(F32) for r in range(WIN)], axis=0)
    halves = [digits[:, k : k + 1] + 256.0 * digits[:, k + 1 : k + 2] for k in range(0, 8, 2)]
    halves = [half.astype(jnp.int32) for half in halves]
    whole = [halves[2 * n + 1] * 65536 + halves[2 * n] for n in range(2)]
    spare = lax.broadcasted_iota(jnp.int32, (KEYS, LANES), 0) % PAD == WIN
    edge_ids = [jnp.where(spare, -1, jnp.where(lane == 0, whole[n], lasts[n])) for n in range(2)]

    def att_a(r, part):
        return jnp.where(late[0] != 0, att_late[r, part, :], att_early[r, part, :])

    def att_upper(r, part):
        return att_b[r, part, :]

    skip = slice(PAD - KEEP, 2 * PAD - KEEP)
    rest = slice(2 * PAD - KEEP - 1, 2 * PAD)
    for n, (first, rows, bias, att) in enumerate(((KEEP, SHIFT, bias_b, att_upper), (0, KEEP, bias_a, att_a))):
        pair = [[side[m, n * WIN + r, skip, :] for r in range(WIN)] for m in range(2)]
        branch = attend(pair, edge_ids[n], first, rows, wqkv, wproj, bias)
        for r in range(rows):
            low, high, place = r * PAD, (rows + r) * PAD, n * SHIFT + r
            rim[0, place, skip, :] = branch[low : low + PAD]
            rim[0, place, rest, :] = att(r, rest)
            rim[1, place, :PAD, :] = att(r, slice(tile_cols, tile_cols + PAD))
            rim[1, place, skip, :] = branch[high : high + PAD]

    narrow = (0.5 * fc2[...].astype(F32)).astype(BF16)
    for r in range(tile_rows):
        middle = slice(2 * PAD, tile_cols)
        inner = att_upper(r, middle) if r < SHIFT else att_a(r - SHIFT, middle)
        pieces = [rim[0, r, PAD:, :], inner, rim[1, r, :PAD, :]]
        summed = own[r].astype(F32) + jnp.concatenate(pieces, axis=0).T
        second = layer_norm(summed, 0).astype(BF16)
        hidden = jnp.dot(fc1[...], second, preferred_element_type=F32)
        hidden = (hidden * (1.0 + lax.erf(hidden * (0.5**0.5)))).astype(BF16)
        out[r] = (summed + jnp.dot(narrow, hidden, preferred_element_type=F32)).astype(BF16)


def shards(features, region_ids, qkv_weight, proj_weight, rel_bias, fc1_weight, fc2_weight):
    tile_rows, tile_cols, width = features.shape
    tile = rowmajor(jnp.swapaxes(features, 1, 2))
    height = lax.axis_size("row")
    slide, row, col = lax.axis_index("slide"), lax.axis_index("row"), lax.axis_index("col")

    def in_wrap(s, r, c):
        return r == 0 or r == height - 1 or (s == 0 and r == 1 and c == 0)

    late = (row >= height - 2) | ((slide == 0) & (row == 0) & (col == 0))
    late = late.astype(jnp.int32).reshape(1)
    onehot = jnp.asarray(bias_onehot(), BF16)
    table = rel_bias.T
    tokens_first = functools.partial(jnp.transpose, axes=(2, 0, 1))
    ids = tokens_first(region_ids)
    att_shape = jax.ShapeDtypeStruct((KEEP, tile_cols + 2 * PAD, width), F32)
    scratch = [
        pltpu.VMEM((WIN, tile_cols + 2 * PAD, width), F32),
        pltpu.VMEM((width, 3 * LANES), BF16),
        pltpu.VMEM((HEADS, PAD, LANES), F32),
        pltpu.VMEM((KEYS, LANES), jnp.int32),
    ]

    def call(kernel, operands, out_shape, scratch_shapes):
        smem, vmem = pl.BlockSpec(memory_space=pltpu.SMEM), pl.BlockSpec(memory_space=pltpu.VMEM)
        return pl.pallas_call(
            kernel,
            out_shape=out_shape,
            in_specs=[smem] + [vmem] * (len(operands) - 1),
            out_specs=jax.tree.map(lambda _: vmem, out_shape),
            scratch_shapes=scratch_shapes,
            compiler_params=pltpu.CompilerParams(vmem_limit_bytes=20 * 1024 * 1024),
        )(*operands)

    before = rowmajor(moved(rowmajor(tile[SHIFT:]), 1, 0))
    ids_before = tokens_first(moved(region_ids, 1, 0))
    after_main = rowmajor(moved(rowmajor(tile[:SHIFT]), -1, 0, lambda s, r, c: not in_wrap(s, r, c)))
    weights = [qkv_weight, proj_weight, table, onehot]
    att = call(early_kernel, [late, tile, after_main, ids, *weights], att_shape, scratch)
    after_wrap = rowmajor(moved(rowmajor(tile[:SHIFT]), -1, 0, in_wrap))
    left, right = call(
        pack_kernel,
        [late, tile, before, after_main, after_wrap, ids, ids_before],
        (
            jax.ShapeDtypeStruct((3 * WIN, PAD, width), BF16),
            jax.ShapeDtypeStruct((2 * WIN, PAD, width), BF16),
        ),
        scratch[-1:],
    )
    left = moved(left, 0, 1)
    right = moved(right, 0, -1)
    late_att = call(late_kernel, [late, tile, after_wrap, ids, *weights], att_shape, scratch)
    upper = jax.ShapeDtypeStruct((SHIFT, tile_cols + 2 * PAD, width), F32)
    att_b = call(upper_kernel, [late, tile, before, ids_before, *weights], upper, scratch)
    result = call(
        final_kernel,
        [late, tile, before, after_main, after_wrap, left, right, ids, ids_before, *weights]
        + [fc1_weight.T, fc2_weight.T, att, late_att, att_b],
        jax.ShapeDtypeStruct((tile_rows, width, tile_cols), BF16),
        [*scratch[1:], pltpu.VMEM((2, 2 * WIN, 2 * PAD, width), F32), pltpu.VMEM((2, WIN, 2 * PAD, width), F32)],
    )
    return jnp.swapaxes(result, 1, 2)


def solution(mesh):
    spec = P(("slide", "row"), "col", None)
    return jax.shard_map(
        shards,
        mesh=mesh,
        in_specs=(spec, spec, P(), P(), P(), P(), P()),
        out_specs=spec,
        check_vma=False,
    )
```
